32 devices in a mesh: batch: 4 (over x, core), space: 8 (over z, y).
Axes of the slice: x: 2, y: 2, z: 4, core: 2. Of those that a mesh axis runs over, the one named last changes fastest.
Arguments:
- inputs: bfloat16 [4, 128, 64, 64, 128], P('batch', 'space'), may hold values from -6 to 6
- cotangent: bfloat16 [4, 128, 64, 64, 128], P('batch', 'space'), may hold values from -6 to 6
- mode_weights: bfloat16 [256, 16, 64, 128], P('space'), may hold values from -1.5 to 1.5
Outputs:
- input_grad: bfloat16 [4, 128, 64, 64, 128], P('batch', 'space')
- weight_grad: float32 [256, 16, 64, 128], P('space')
The draws below stay inside these ranges and needn't reach their ends.
All inputs are finite; a program needn't handle non-finite values.
Results may differ from the reference program's by a relative error of at most 0.015.
Values may be sent and summed in bfloat16 or wider, within the bound.
No kernel may reach another device: no remote copies, remote signals or barrier semaphores. Data moves between devices by JAX's collectives and lax.ppermute only.
A program may use at most 192 MiB of HBM per device.

```python
import math
import jax
import jax.numpy as jnp
from jax import lax

C = 64
X = 64
Y = 128
Z = 128
MX = 16
MY = 16
MZ = 16
PAIRS = 256
B = 4


def shard_levels(key, shape, pieces, low, high):
    gain, own = 1.0, jax.random.fold_in(key, 6)
    for position, parts in pieces:
        steps = jnp.exp(jax.random.uniform(jax.random.fold_in(own, position), (parts,), jnp.float32, low / len(pieces), high / len(pieces)))
        gain = gain * jnp.repeat(steps, shape[position] // parts).reshape([-1 if axis == position else 1 for axis in range(len(shape))])
    return gain


def bell_draw(key, dims, deviation, bound, pieces=(), kind=jnp.bfloat16):
    gain = shard_levels(key, dims, pieces, -0.22, 0.18) if pieces else 1.0
    array = jax.random.normal(key, dims, jnp.float32) * deviation * gain
    return jnp.minimum(jnp.maximum(array, -bound), bound).astype(kind)


def setup_inputs(seed: int = 0) -> dict:
    splits = jax.random.split(jax.random.key(seed), 4)
    return {
        "inputs": bell_draw(splits[0], (B, Y, C, X, Z), 1.0, 6.0, ((0, 4), (1, 8))),
        "cotangent": bell_draw(splits[1], (B, Y, C, X, Z), 1.0, 6.0, ((0, 4), (1, 8))),
        "mode_weights": bell_draw(splits[2], (PAIRS, MY, C, 2 * C), 0.25, 1.5, ((0, 8),)),
    }


two_pi = 2.0 * math.pi
highest = lax.Precision.HIGHEST

def twiddles(wave_list, positions, length):
    product = wave_list[:, None] * positions[None, :] % length
    angles = two_pi / length * product.astype(jnp.float32)
    return (jnp.cos(angles), jnp.sin(angles))

def wave_pair(retained, length):
    return jnp.concatenate([jnp.arange(retained // 2), jnp.arange(length - retained // 2, length)]).astype(jnp.int32)

def plane_spectrum(values, z_table, cos_x, sin_x, factor):
    lead_dims = values.shape[:-3]
    along_z = jnp.dot(values.reshape(-1, Z), z_table, preferred_element_type=jnp.float32)
    along_z = along_z.reshape(lead_dims + (C, X, 2 * MZ))
    first_term = jnp.einsum('kx,...cxm->...ckm', cos_x, along_z, precision=highest)
    second_term = jnp.einsum('kx,...cxm->...ckm', sin_x, along_z, precision=highest)
    real_part = (first_term[..., :MZ] + second_term[..., MZ:]) * factor
    imag_part = (first_term[..., MZ:] - second_term[..., :MZ]) * factor
    stacked = jnp.stack([real_part, imag_part], axis=-4)
    return stacked.reshape(lead_dims + (2, C, MX * MZ)).astype(jnp.bfloat16)

def modes_along_y(spectra, cos_y, sin_y):
    values_f = spectra.astype(jnp.float32)
    real_in = values_f[:, :, 0]
    imag_in = values_f[:, :, 1]
    real_out = jnp.einsum('ky,bycp->pbkc', cos_y, real_in, precision=highest) + jnp.einsum('ky,bycp->pbkc', sin_y, imag_in, precision=highest)
    imag_out = jnp.einsum('ky,bycp->pbkc', cos_y, imag_in, precision=highest) - jnp.einsum('ky,bycp->pbkc', sin_y, real_in, precision=highest)
    return jnp.stack([real_out, imag_out], axis=3)

def planes_along_y(mode_data, cos_y, sin_y):
    values_f = mode_data.astype(jnp.float32)
    real_in = values_f[:, :, :, 0]
    imag_in = values_f[:, :, :, 1]
    real_out = jnp.einsum('ky,pbkc->bycp', cos_y, real_in, precision=highest) - jnp.einsum('ky,pbkc->bycp', sin_y, imag_in, precision=highest)
    imag_out = jnp.einsum('ky,pbkc->bycp', sin_y, real_in, precision=highest) + jnp.einsum('ky,pbkc->bycp', cos_y, imag_in, precision=highest)
    return jnp.stack([real_out, imag_out], axis=2)

def plane_inverse(spectra, cos_x, sin_x, z_back):
    lead_dims = spectra.shape[:-3]
    values_f = spectra.astype(jnp.float32).reshape(lead_dims + (2, C, MX, MZ))
    real_in = values_f[..., 0, :, :, :]
    imag_in = values_f[..., 1, :, :, :]
    real_out = jnp.einsum('kx,...ckm->...cxm', cos_x, real_in, precision=highest) - jnp.einsum('kx,...ckm->...cxm', sin_x, imag_in, precision=highest)
    imag_out = jnp.einsum('kx,...ckm->...cxm', sin_x, real_in, precision=highest) + jnp.einsum('kx,...ckm->...cxm', cos_x, imag_in, precision=highest)
    joined = jnp.concatenate([real_out, imag_out], axis=-1)
    result = jnp.dot(joined.reshape(-1, 2 * MZ), z_back, precision=highest, preferred_element_type=jnp.float32)
    return result.reshape(lead_dims + (C, X, Z)).astype(jnp.bfloat16)

def split_cot(cot_modes):
    real_part = cot_modes[:, :, :, 0]
    imag_part = cot_modes[:, :, :, 1]
    return (jnp.concatenate([real_part, imag_part], axis=-1), jnp.concatenate([imag_part, -real_part], axis=-1))

def reference(inputs, cotangent, mode_weights):
    inv_scale = 1.0 / math.sqrt(X * Y * Z)
    cos_z, sin_z = twiddles(jnp.arange(MZ).astype(jnp.int32), jnp.arange(Z).astype(jnp.int32), Z)
    z_table = jnp.concatenate([cos_z.T, -sin_z.T], axis=1).astype(jnp.bfloat16)
    z_back = jnp.concatenate([cos_z, -sin_z], axis=0) * inv_scale
    cos_x, sin_x = twiddles(wave_pair(MX, X), jnp.arange(X).astype(jnp.int32), X)
    cos_y, sin_y = twiddles(wave_pair(MY, Y), jnp.arange(Y).astype(jnp.int32), Y)
    plain_z = jnp.full((MZ,), inv_scale, jnp.float32)
    weight_z = jnp.where(jnp.arange(MZ) == 0, 1.0, 2.0).astype(jnp.float32) * inv_scale

    def per_sample(sample):
        values, cot_values = sample
        spec_in = plane_spectrum(values[None], z_table, cos_x, sin_x, plain_z)
        spec_cot = plane_spectrum(cot_values[None], z_table, cos_x, sin_x, weight_z)
        return (modes_along_y(spec_in, cos_y, sin_y)[:, 0], modes_along_y(spec_cot, cos_y, sin_y)[:, 0])
    input_modes, cot_modes = lax.map(per_sample, (inputs, cotangent))
    input_modes = jnp.transpose(input_modes, (1, 0, 2, 3, 4)).astype(jnp.bfloat16)
    cot_modes = jnp.transpose(cot_modes, (1, 0, 2, 3, 4)).astype(jnp.bfloat16)
    cot_one, cot_two = split_cot(cot_modes)
    cot_one = cot_one.astype(jnp.float32)
    cot_two = cot_two.astype(jnp.float32)
    input_f = input_modes.astype(jnp.float32)
    weight_grad = jnp.einsum('pbki,pbkj->pkij', input_f[:, :, :, 0], cot_one) + jnp.einsum('pbki,pbkj->pkij', input_f[:, :, :, 1], cot_two)
    weights_f = mode_weights.astype(jnp.float32)
    grad_real = jnp.einsum('pbkj,pkij->pbki', cot_one, weights_f)
    grad_imag = jnp.einsum('pbkj,pkij->pbki', cot_two, weights_f)
    mode_grad = jnp.stack([grad_real, grad_imag], axis=3).astype(jnp.bfloat16)

    def back_sample(sample_modes):
        planes = planes_along_y(sample_modes[:, None], cos_y, sin_y).astype(jnp.bfloat16)
        return plane_inverse(planes, cos_x, sin_x, z_back)[0]
    input_grad = lax.map(back_sample, jnp.transpose(mode_grad, (1, 0, 2, 3, 4)))
    return (input_grad, weight_grad)
```

```python
import functools
import math

import jax
import jax.numpy as jnp
import numpy as np
from jax import lax
from jax.experimental import pallas as pl
from jax.experimental.pallas import tpu as pltpu
from jax.sharding import PartitionSpec as P

C = 64
X = 64
Y = 128
Z = 128
MX = 16
MY = 16
MZ = 16


two_pi = 2.0 * math.pi
highest = lax.Precision.HIGHEST


def twiddles(wave_list, positions, length):
    product = wave_list[:, None] * positions[None, :] % length
    angles = two_pi / length * product.astype(jnp.float32)
    return (jnp.cos(angles), jnp.sin(angles))


def wave_pair(retained, length):
    return jnp.concatenate([jnp.arange(retained // 2), jnp.arange(length - retained // 2, length)])


def plane_spectrum(values, z_table, cos_x, sin_x, factor):
    lead_dims = values.shape[:-3]
    along_z = jnp.dot(values.reshape(-1, Z), z_table, preferred_element_type=jnp.float32)
    along_z = along_z.reshape(lead_dims + (C, X, 2 * MZ))
    first_term = jnp.einsum("kx,...cxm->...ckm", cos_x, along_z, precision=highest)
    second_term = jnp.einsum("kx,...cxm->...ckm", sin_x, along_z, precision=highest)
    real_part = (first_term[..., :MZ] + second_term[..., MZ:]) * factor
    imag_part = (first_term[..., MZ:] - second_term[..., :MZ]) * factor
    stacked = jnp.stack([real_part, imag_part], axis=-4)
    return stacked.reshape(lead_dims + (2, C, MX * MZ)).astype(jnp.bfloat16)


def modes_along_y(spectra, cos_y, sin_y):
    values_f = spectra.astype(jnp.float32)
    real_in = values_f[:, :, 0]
    imag_in = values_f[:, :, 1]
    real_out = jnp.einsum("ky,bycp->pbkc", cos_y, real_in, precision=highest) + jnp.einsum(
        "ky,bycp->pbkc", sin_y, imag_in, precision=highest
    )
    imag_out = jnp.einsum("ky,bycp->pbkc", cos_y, imag_in, precision=highest) - jnp.einsum(
        "ky,bycp->pbkc", sin_y, real_in, precision=highest
    )
    return jnp.stack([real_out, imag_out], axis=3)


def planes_along_y(mode_data, cos_y, sin_y):
    values_f = mode_data.astype(jnp.float32)
    real_in = values_f[:, :, :, 0]
    imag_in = values_f[:, :, :, 1]
    real_out = jnp.einsum("ky,pbkc->bycp", cos_y, real_in, precision=highest) - jnp.einsum(
        "ky,pbkc->bycp", sin_y, imag_in, precision=highest
    )
    imag_out = jnp.einsum("ky,pbkc->bycp", sin_y, real_in, precision=highest) + jnp.einsum(
        "ky,pbkc->bycp", cos_y, imag_in, precision=highest
    )
    return jnp.stack([real_out, imag_out], axis=2)


def plane_inverse(spectra, cos_x, sin_x, z_back):
    lead_dims = spectra.shape[:-3]
    values_f = spectra.astype(jnp.float32).reshape(lead_dims + (2, C, MX, MZ))
    real_in = values_f[..., 0, :, :, :]
    imag_in = values_f[..., 1, :, :, :]
    real_out = jnp.einsum("kx,...ckm->...cxm", cos_x, real_in, precision=highest) - jnp.einsum(
        "kx,...ckm->...cxm", sin_x, imag_in, precision=highest
    )
    imag_out = jnp.einsum("kx,...ckm->...cxm", sin_x, real_in, precision=highest) + jnp.einsum(
        "kx,...ckm->...cxm", cos_x, imag_in, precision=highest
    )
    joined = jnp.concatenate([real_out, imag_out], axis=-1)
    result = jnp.dot(
        joined.reshape(-1, 2 * MZ), z_back, precision=highest, preferred_element_type=jnp.float32
    )
    return result.reshape(lead_dims + (C, X, Z)).astype(jnp.bfloat16)


def split_cot(cot_modes):
    real_part = cot_modes[:, :, :, 0]
    imag_part = cot_modes[:, :, :, 1]
    return (
        jnp.concatenate([real_part, imag_part], axis=-1),
        jnp.concatenate([imag_part, -real_part], axis=-1),
    )


def weight_terms(input_modes, cot_modes):
    cot_one, cot_two = split_cot(cot_modes)
    first_term = jnp.einsum(
        "pbki,pbkj->pkij", input_modes[:, :, :, 0], cot_one, preferred_element_type=jnp.float32
    )
    second_term = jnp.einsum(
        "pbki,pbkj->pkij", input_modes[:, :, :, 1], cot_two, preferred_element_type=jnp.float32
    )
    return first_term + second_term


def local_any(inputs, cotangent, mode_weights):
    inv_scale = 1.0 / math.sqrt(X * Y * Z)
    cos_z, sin_z = twiddles(jnp.arange(MZ), jnp.arange(Z), Z)
    z_table = jnp.concatenate([cos_z.T, -sin_z.T], axis=1).astype(jnp.bfloat16)
    z_back = jnp.concatenate([cos_z, -sin_z], axis=0) * inv_scale
    cos_x, sin_x = twiddles(wave_pair(MX, X), jnp.arange(X), X)
    plain_z = jnp.full((MZ,), inv_scale, jnp.float32)
    weight_z = jnp.where(jnp.arange(MZ) == 0, 1.0, 2.0).astype(jnp.float32) * inv_scale
    input_spec = plane_spectrum(inputs, z_table, cos_x, sin_x, plain_z)
    cot_spec = plane_spectrum(cotangent, z_table, cos_x, sin_x, weight_z)
    y_waves = wave_pair(MY, Y)
    positions = jnp.arange(Y)
    cos_y, sin_y = twiddles(y_waves, positions, Y)
    moved_input, moved_cot = (
        lax.all_to_all(input_spec, "space", split_axis=4, concat_axis=1, tiled=True),
        lax.all_to_all(cot_spec, "space", split_axis=4, concat_axis=1, tiled=True),
    )
    input_modes = modes_along_y(moved_input, cos_y, sin_y)
    cot_modes = modes_along_y(moved_cot, cos_y, sin_y)
    input_modes = input_modes.astype(jnp.bfloat16)
    cot_modes = cot_modes.astype(jnp.bfloat16)
    weight_grad = lax.psum(
        weight_terms(input_modes, cot_modes).astype(jnp.bfloat16), "batch"
    ).astype(jnp.float32)
    cot_one, cot_two = split_cot(cot_modes)
    grad_real = jnp.einsum(
        "pbkj,pkij->pbki", cot_one, mode_weights, preferred_element_type=jnp.float32
    )
    grad_imag = jnp.einsum(
        "pbkj,pkij->pbki", cot_two, mode_weights, preferred_element_type=jnp.float32
    )
    mode_grad = jnp.stack([grad_real, grad_imag], axis=3).astype(jnp.bfloat16)
    plane_modes = planes_along_y(mode_grad, cos_y, sin_y).astype(jnp.bfloat16)
    back_spec = lax.all_to_all(plane_modes, "space", split_axis=1, concat_axis=4, tiled=True)
    input_grad = plane_inverse(back_spec, cos_x, sin_x, z_back)
    return (input_grad, weight_grad)


GROUP = 8
ROWS = 16
LANES = 128
BLOCK = 4
STEP = 4


def angles_of(waves, length):
    turns = 2.0 * np.pi / length * (np.outer(waves, np.arange(length)) % length)
    return np.cos(turns), np.sin(turns)


def signed_waves(retained, length):
    return np.concatenate([np.arange(retained // 2), np.arange(length - retained // 2, length)])


def as_table(array):
    return np.asarray(array, np.float32).astype(jnp.bfloat16)


def x_tables(length):
    cos_x, sin_x = angles_of(signed_waves(MX, length), length)
    unit = np.eye(GROUP)
    both = np.stack([cos_x, sin_x])
    forward = np.einsum("qkx,cd->qkcdx", both, unit).reshape(2 * MX * GROUP, GROUP * length)
    both = np.stack([cos_x, -sin_x])
    back = np.einsum("qkx,cd->dxqkc", both, unit).reshape(GROUP * length, 2 * MX * GROUP)
    return as_table(forward), as_table(back)


def z_tables(length, scale):
    cos_z, sin_z = angles_of(np.arange(MZ), length)
    forward = np.concatenate(
        [np.concatenate([cos_z, -sin_z], axis=1), np.concatenate([-sin_z, -cos_z], axis=1)]
    )
    doubled = np.where(np.arange(MZ) == 0, 1.0, 2.0)[:, None]
    doubled = np.concatenate([doubled, doubled])
    back = np.concatenate(
        [np.concatenate([cos_z, sin_z], axis=1), np.concatenate([-sin_z, cos_z], axis=1)]
    )
    return (
        as_table(as_table(forward).astype(np.float32) * scale),
        as_table(as_table(forward).astype(np.float32) * scale * doubled),
        as_table(back * scale),
    )


def y_tables(length, shards):
    cos_y, sin_y = angles_of(signed_waves(MY, length), length)
    per = length // shards
    real = np.stack([cos_y, sin_y], axis=1)
    imag = np.stack([-sin_y, cos_y], axis=1)
    rows = np.stack([real, imag], axis=1).reshape(2 * MY, 2, shards, per)
    forward = rows.transpose(2, 0, 1, 3).reshape(shards, 2 * MY, 2 * per)
    back = np.stack([np.stack([cos_y, -sin_y], axis=-1), np.stack([sin_y, cos_y], axis=-1)])
    back = back.transpose(2, 0, 1, 3).reshape(shards, 2 * per, 2 * MY)
    return as_table(forward), as_table(back)


def peer_order(bits):
    if not bits:
        return [0]
    kept = peer_order(bits[1:])
    return kept + [distance ^ bits[0] for distance in kept]


def gathered_order(bits):
    held = [0]
    for bit in bits:
        held = held + [distance ^ bit for distance in held]
    return held


def dot(left, right, left_dim=1, right_dim=0):
    dims = (((left_dim,), (right_dim,)), ((), ()))
    return lax.dot_general(left, right, dims, preferred_element_type=jnp.float32)


def spectrum_kernel(
    planes, orders, me_ref, field_ref, x_ref, z_ref, y_ref, *refs
):
    step = pl.program_id(0)
    block, channels, length, depth = field_ref.shape[1:]
    *part_refs, rows_ref, total_ref = refs
    shards, _, width = total_ref.shape
    for plane in range(block):
        for first in range(0, channels, 2 * GROUP):
            sides = [
                field_ref[0, plane, first + side * GROUP : first + (side + 1) * GROUP].reshape(
                    GROUP * length, depth
                )
                for side in range(2)
            ]
            mixed = dot(x_ref[...], jnp.concatenate(sides, axis=1))
            half = MX * GROUP
            parts = [
                jnp.concatenate(
                    [
                        mixed[:half, side * depth : (side + 1) * depth],
                        mixed[half:, side * depth : (side + 1) * depth],
                    ],
                    axis=1,
                ).reshape(MX, GROUP, 2 * depth)
                for side in range(2)
            ]
            rows_ref[plane, :, first : first + 2 * GROUP, :] = jnp.concatenate(
                parts, axis=1
            ).astype(jnp.bfloat16)
        modes = dot(z_ref[...], rows_ref[plane].reshape(MX * channels, 2 * depth), 1, 1)
        for shard in range(shards):
            total_ref[shard, pl.ds(step * block + plane, 2 * MZ, stride=planes), :] = modes[
                :, shard * width : (shard + 1) * width
            ]

    @pl.when(step == pl.num_programs(0) - 1)
    def _():
        me = me_ref[0]
        table = y_ref[me]
        chunk = MZ // len(orders)
        for stream, order in enumerate(orders):
            for kz in range(chunk):
                first = (stream * chunk + kz) * planes
                parts = [
                    jnp.concatenate(
                        [
                            total_ref[me ^ distance, pl.ds(part * MZ * planes + first, planes), :]
                            for distance in order
                        ],
                        axis=1,
                    )
                    for part in range(2)
                ]
                modes = dot(table, jnp.concatenate(parts).astype(jnp.bfloat16))
                modes = modes.astype(jnp.bfloat16)
                for place in range(shards):
                    side, place_in = divmod(place, shards // 2)
                    part_refs[2 * stream + side][place_in, kz] = modes[
                        :, place * width : (place + 1) * width
                    ]


def plane_modes(me, field, x_table, z_table, y_table, orders, block):
    _, planes, channels, length, depth = field.shape
    shards = len(orders[0])
    width = MX * channels // shards
    shape = (shards // 2, MZ // len(orders), 2 * MY, width)
    whole = pl.BlockSpec(shape, lambda i: (0, 0, 0, 0))
    return pl.pallas_call(
        functools.partial(spectrum_kernel, planes, orders),
        out_shape=[jax.ShapeDtypeStruct(shape, jnp.bfloat16)] * (2 * len(orders)),
        grid=(planes // block,),
        in_specs=[
            pl.BlockSpec(memory_space=pltpu.SMEM),
            pl.BlockSpec((1, block, channels, length, depth), lambda i: (0, i, 0, 0, 0)),
            pl.BlockSpec(x_table.shape, lambda i: (0, 0)),
            pl.BlockSpec(z_table.shape, lambda i: (0, 0)),
            pl.BlockSpec(y_table.shape, lambda i: (0, 0, 0)),
        ],
        out_specs=[whole] * (2 * len(orders)),
        scratch_shapes=[
            pltpu.VMEM((block, MX, channels, 2 * depth), jnp.bfloat16),
            pltpu.VMEM((shards, 2 * MZ * planes, width), jnp.float32),
        ],
        compiler_params=pltpu.CompilerParams(dimension_semantics=("arbitrary",)),
        cost_estimate=pl.CostEstimate(
            flops=2 * field.size * 8 * MX, bytes_accessed=2 * field.size, transcendentals=0
        ),
        name="plane_modes",
    )(me, field, x_table, z_table, y_table)


def swapped(array, bit, shards):
    return lax.ppermute(array, "space", [(i, i ^ bit) for i in range(shards)])


def total(keep, moved):
    return (keep.astype(jnp.float32) + moved.astype(jnp.float32)).astype(jnp.bfloat16)


def halved(keep, moved):
    both = total(keep, moved)
    half = both.shape[0] // 2
    return both[:half], both[half:]


def after(values):
    return lax.optimization_barrier(values)


def turned_rows(modes):
    rows = modes.shape[0]
    row = lax.broadcasted_iota(jnp.int32, modes.shape, 0)
    return jnp.where(row % 2 == 0, pltpu.roll(modes, rows - 1, 0), -pltpu.roll(modes, 1, 0))


def join_halves(plain, turned, side):
    low = lax.broadcasted_iota(jnp.int32, plain.shape, 1) < LANES // 2
    if side == 0:
        return jnp.where(low, plain, pltpu.roll(turned, LANES // 2, 1))
    return jnp.where(low, pltpu.roll(plain, LANES // 2, 1), turned)


def mode_grad_kernel(keep_ref, moved_ref, w_ref, modes_ref, grad_ref):
    _, chunk, _, channels, _ = w_ref.shape
    row = lax.broadcasted_iota(jnp.int32, (2 * MY, MY * channels), 0) // 2
    lane = lax.broadcasted_iota(jnp.int32, (2 * MY, MY * channels), 1) // channels
    own = row == lane
    low = lax.broadcasted_iota(jnp.int32, (2 * MY, LANES), 1) < LANES // 2
    for kz in range(chunk):
        plain = keep_ref[0, kz].astype(jnp.float32) + moved_ref[0, kz].astype(jnp.float32)
        turned = turned_rows(plain)
        modes_ref[kz] = plain.astype(jnp.bfloat16)
        sides = []
        for side in range(2):
            left = join_halves(plain, turned, side).astype(jnp.bfloat16)
            crossed = dot(left, w_ref[side, kz].reshape(MY * channels, 2 * channels), 1, 1)
            crossed = jnp.where(own, crossed, 0.0)
            kept = crossed[:, :LANES]
            for first in range(LANES, MY * channels, LANES):
                kept = kept + crossed[:, first : first + LANES]
            sides.append(kept + pltpu.roll(kept, LANES // 2, 1))
        grad_ref[0, kz] = jnp.where(low, sides[0], sides[1]).astype(jnp.bfloat16)


def mode_grads(keep, moved, weights, first, chunk):
    _, kinds, rows, width = keep.shape
    channels = weights.shape[3]
    part_spec = pl.BlockSpec((1, chunk, rows, width), lambda i: (0, i, 0, 0))
    return pl.pallas_call(
        mode_grad_kernel,
        out_shape=(
            jax.ShapeDtypeStruct(keep.shape[1:], jnp.bfloat16),
            jax.ShapeDtypeStruct(keep.shape, jnp.bfloat16),
        ),
        grid=(kinds // chunk,),
        in_specs=[
            part_spec,
            part_spec,
            pl.BlockSpec(
                (2, chunk, MY, channels, 2 * channels), lambda i: (0, i + first // chunk, 0, 0, 0)
            ),
        ],
        out_specs=(pl.BlockSpec((chunk, rows, width), lambda i: (i, 0, 0)), part_spec),
        compiler_params=pltpu.CompilerParams(dimension_semantics=("arbitrary",)),
        cost_estimate=pl.CostEstimate(
            flops=4 * MY * weights.size, bytes_accessed=weights.size, transcendentals=0
        ),
        name="mode_grads",
    )(keep, moved, weights)


def weight_kernel(channels, *refs):
    *mode_refs, out_ref = refs
    samples = len(mode_refs) // 2
    for kz in range(out_ref.shape[1]):
        inputs = jnp.concatenate([ref[kz] for ref in mode_refs[:samples]]).astype(jnp.float32)
        cots = jnp.concatenate([ref[kz] for ref in mode_refs[samples:]]).astype(jnp.float32)
        turned = turned_rows(cots)
        wave = lax.broadcasted_iota(jnp.int32, cots.shape, 0) % (2 * MY) // 2
        left = inputs.T.astype(jnp.bfloat16)
        for side in range(2):
            right = join_halves(cots, turned, side)
            mine = left[side * channels : (side + 1) * channels]
            for ky in range(0, MY, 2):
                pair = [jnp.where(wave == ky + k, right, 0.0).astype(jnp.bfloat16) for k in range(2)]
                grads = dot(mine, jnp.concatenate(pair, axis=1))
                for k in range(2):
                    out_ref[side, kz, ky + k] = grads[:, k * LANES : (k + 1) * LANES]


def weight_grads(input_modes, cot_modes, channels, chunk):
    samples = len(input_modes)
    kinds, rows, width = input_modes[0].shape
    shape = (2, kinds, MY, channels, 2 * channels)
    return pl.pallas_call(
        functools.partial(weight_kernel, channels),
        out_shape=jax.ShapeDtypeStruct(shape, jnp.float32),
        grid=(kinds // chunk,),
        in_specs=[pl.BlockSpec((chunk, rows, width), lambda i: (i, 0, 0))] * (2 * samples),
        out_specs=pl.BlockSpec((2, chunk, MY, channels, 2 * channels), lambda i: (0, i, 0, 0, 0)),
        compiler_params=pltpu.CompilerParams(dimension_semantics=("arbitrary",)),
        cost_estimate=pl.CostEstimate(
            flops=2 * 128 * math.prod(shape), bytes_accessed=4 * math.prod(shape), transcendentals=0
        ),
        name="weight_grads",
    )(*input_modes, *cot_modes)


def inverse_kernel(orders, me_ref, *refs):
    *held_refs, y_ref, z_ref, x_ref, out_ref, total_ref = refs
    step = pl.program_id(0)
    block, channels, length, depth = out_ref.shape[1:]
    shards, _, width = total_ref.shape

    @pl.when(step == 0)
    def _():
        me = me_ref[0]
        table = y_ref[me]
        chunk = MZ // len(orders)
        for stream, order in enumerate(orders):
            for kz in range(chunk):
                modes = jnp.concatenate(
                    [
                        ref[place, kz]
                        for ref in held_refs[2 * stream : 2 * stream + 2]
                        for place in range(shards // 2)
                    ],
                    axis=1,
                )
                spread = dot(table, modes)
                for place, distance in enumerate(order):
                    rows = pl.ds(stream * chunk + kz, table.shape[0], stride=MZ)
                    total_ref[me ^ distance, rows, :] = spread[
                        :, place * width : (place + 1) * width
                    ]

    for plane in range(block):
        rows = pl.ds((step * block + plane) * 2 * MZ, 2 * MZ)
        modes = jnp.concatenate([total_ref[shard, rows, :] for shard in range(shards)], axis=1)
        modes = modes.astype(jnp.bfloat16)
        along = dot(modes, z_ref[...], 0, 0).reshape(MX, channels, 2 * depth)
        for first in range(0, channels, 2 * GROUP):
            sides = []
            for side in range(2):
                start = first + side * GROUP
                piece = along[:, start : start + GROUP].reshape(MX * GROUP, 2 * depth)
                sides.append(jnp.concatenate([piece[:, :depth], piece[:, depth:]], axis=0))
            grads = dot(x_ref[...], jnp.concatenate(sides, axis=1).astype(jnp.bfloat16))
            for side in range(2):
                start = first + side * GROUP
                out_ref[0, plane, start : start + GROUP] = (
                    grads[:, side * depth : (side + 1) * depth]
                    .reshape(GROUP, length, depth)
                    .astype(jnp.bfloat16)
                )


def plane_grads(me, held, y_back, z_back, x_back, orders, shape, block):
    _, planes, channels, length, depth = shape
    shards = len(orders[0])
    width = held[0].shape[-1]
    return pl.pallas_call(
        functools.partial(inverse_kernel, orders),
        out_shape=jax.ShapeDtypeStruct(shape, jnp.bfloat16),
        grid=(planes // block,),
        in_specs=[pl.BlockSpec(memory_space=pltpu.SMEM)]
        + [pl.BlockSpec(array.shape, lambda i: (0, 0, 0, 0)) for array in held]
        + [
            pl.BlockSpec(y_back.shape, lambda i: (0, 0, 0)),
            pl.BlockSpec(z_back.shape, lambda i: (0, 0)),
            pl.BlockSpec(x_back.shape, lambda i: (0, 0)),
        ],
        out_specs=pl.BlockSpec((1, block, channels, length, depth), lambda i: (0, i, 0, 0, 0)),
        scratch_shapes=[pltpu.VMEM((shards, planes * 2 * MZ, width), jnp.float32)],
        compiler_params=pltpu.CompilerParams(dimension_semantics=("arbitrary",)),
        cost_estimate=pl.CostEstimate(
            flops=2 * math.prod(shape) * 8 * MX,
            bytes_accessed=2 * math.prod(shape),
            transcendentals=0,
        ),
        name="plane_grads",
    )(me, *held, y_back, z_back, x_back)


def from_peers(array, groups):
    others = [
        lax.ppermute(array, "batch", [(i, i ^ k) for i in range(groups)]) for k in range(1, groups)
    ]
    return [array] + others


def local_fast(shards, groups, inputs, cotangent, mode_weights):
    _, planes, channels, length, depth = inputs.shape
    scale = 1.0 / math.sqrt(length * planes * shards * depth)
    x_table, x_back = x_tables(length)
    z_plain, z_double, z_back = z_tables(depth, scale)
    y_table, y_back = y_tables(planes * shards, shards)
    me = lax.axis_index("space").reshape(1)
    bits = [1 << place for place in range(shards.bit_length() - 1)]
    paths = [bits, [bits[1], bits[0]] + bits[2:]]
    down = [peer_order(path) for path in paths]
    up = [gathered_order(path[::-1]) for path in paths]
    streams = range(len(paths))

    def split(parts):
        return [parts[2 * k] for k in streams], [parts[2 * k + 1] for k in streams]

    def reduce_step(keep, moved):
        pairs = [halved(keep[k], moved[k]) for k in streams]
        return [pair[0] for pair in pairs], [pair[1] for pair in pairs]

    def swap_all(arrays, routes, step):
        return [swapped(arrays[k], routes[k][step], shards) for k in streams]

    keep, send = split(plane_modes(me, cotangent, x_table, z_double, y_table, down, BLOCK))
    moved = swap_all(send, paths, 0)
    parts = plane_modes(me, inputs, x_table, z_plain, y_table, down, BLOCK)
    moved, parts = after((moved, parts))
    input_keep, input_send = split(parts)
    input_moved, input_sends = None, 0
    for step in range(1, len(bits)):
        keep, send = reduce_step(keep, moved)
        if input_moved is None:
            send, input_send = after((send, input_send))
        else:
            send, input_moved = after((send, input_moved))
            input_keep, input_send = reduce_step(input_keep, input_moved)
        moved = swap_all(send, paths, step)
        input_moved = swap_all(input_send, paths, input_sends)
        input_sends += 1
    weights = mode_weights.reshape(2, MZ, MY, channels, 2 * channels)
    chunk = MZ // len(paths)
    cot_modes, held = [], []
    for k in streams:
        if k:
            keep[k], cot_modes[-1] = after((keep[k], cot_modes[-1]))
        else:
            keep[k], input_send = after((keep[k], input_send))
        modes, grad = mode_grads(keep[k], moved[k], weights, k * chunk, STEP)
        cot_modes.append(modes)
        held.append(grad)
    routes = [path[::-1] for path in paths]
    came = swap_all(held, routes, 0)
    while input_sends < len(bits):
        input_moved, cot_modes[-1] = after((input_moved, cot_modes[-1]))
        input_keep, input_send = reduce_step(input_keep, input_moved)
        input_moved = swap_all(input_send, paths, input_sends)
        input_sends += 1
    all_cots = from_peers(jnp.concatenate(cot_modes), groups)
    input_modes = None
    for step in range(1, len(bits)):
        held = [jnp.concatenate([held[k], came[k]]) for k in streams]
        came = swap_all(held, routes, step)
        if step == 1:
            input_moved, held = after((input_moved, held))
            input_modes = jnp.concatenate([total(input_keep[k][0], input_moved[k][0]) for k in streams])
            all_inputs = from_peers(input_modes, groups)
    all_inputs, held = after((all_inputs, held))
    weight_grad = weight_grads(all_inputs, all_cots, channels, STEP)
    came, weight_grad = after((came, weight_grad))
    gathered = [array for k in streams for array in (held[k], came[k])]
    input_grad = plane_grads(
        me, gathered, y_back, z_back, x_back, up, inputs.shape, BLOCK
    )
    return (input_grad, weight_grad.reshape(mode_weights.shape))


def local(shards, groups, inputs, cotangent, mode_weights):
    samples, planes, channels, _, depth = inputs.shape
    fits = (
        samples == 1
        and planes % ROWS == 0
        and MX % shards == 0
        and MX // shards * channels == LANES
        and depth == LANES
        and shards > 2
        and shards & (shards - 1) == 0
        and groups & (groups - 1) == 0
    )
    if fits:
        return local_fast(shards, groups, inputs, cotangent, mode_weights)
    return local_any(inputs, cotangent, mode_weights)


def solution(mesh):
    placed = (
        P("batch", "space", None, None, None),
        P("batch", "space", None, None, None),
        P("space", None, None, None),
    )
    return jax.shard_map(
        functools.partial(local, mesh.shape["space"], mesh.shape["batch"]),
        mesh=mesh,
        in_specs=placed,
        out_specs=(P("batch", "space", None, None, None), P("space", None, None, None)),
        check_vma=False,
    )
```

```python
import functools
import math

import jax
import jax.numpy as jnp
import numpy as np
from jax import lax
from jax.experimental import pallas as pl
from jax.experimental.pallas import tpu as pltpu
from jax.sharding import PartitionSpec as P


C = 64
X = 64
Y = 128
Z = 128
MX = 16
MY = 16
MZ = 16


two_pi = 2.0 * math.pi
highest = lax.Precision.HIGHEST


def twiddles(wave_list, positions, length):
    product = wave_list[:, None] * positions[None, :] % length
    angles = two_pi / length * product.astype(jnp.float32)
    return (jnp.cos(angles), jnp.sin(angles))


def wave_pair(retained, length):
    return jnp.concatenate([jnp.arange(retained // 2), jnp.arange(length - retained // 2, length)])


def plane_spectrum(values, z_table, cos_x, sin_x, factor):
    lead_dims = values.shape[:-3]
    along_z = jnp.dot(values.reshape(-1, Z), z_table, preferred_element_type=jnp.float32)
    along_z = along_z.reshape(lead_dims + (C, X, 2 * MZ))
    first_term = jnp.einsum("kx,...cxm->...ckm", cos_x, along_z, precision=highest)
    second_term = jnp.einsum("kx,...cxm->...ckm", sin_x, along_z, precision=highest)
    real_part = (first_term[..., :MZ] + second_term[..., MZ:]) * factor
    imag_part = (first_term[..., MZ:] - second_term[..., :MZ]) * factor
    stacked = jnp.stack([real_part, imag_part], axis=-4)
    return stacked.reshape(lead_dims + (2, C, MX * MZ)).astype(jnp.bfloat16)


def modes_along_y(spectra, cos_y, sin_y):
    values_f = spectra.astype(jnp.float32)
    real_in = values_f[:, :, 0]
    imag_in = values_f[:, :, 1]
    real_out = jnp.einsum("ky,bycp->pbkc", cos_y, real_in, precision=highest) + jnp.einsum(
        "ky,bycp->pbkc", sin_y, imag_in, precision=highest
    )
    imag_out = jnp.einsum("ky,bycp->pbkc", cos_y, imag_in, precision=highest) - jnp.einsum(
        "ky,bycp->pbkc", sin_y, real_in, precision=highest
    )
    return jnp.stack([real_out, imag_out], axis=3)


def planes_along_y(mode_data, cos_y, sin_y):
    values_f = mode_data.astype(jnp.float32)
    real_in = values_f[:, :, :, 0]
    imag_in = values_f[:, :, :, 1]
    real_out = jnp.einsum("ky,pbkc->bycp", cos_y, real_in, precision=highest) - jnp.einsum(
        "ky,pbkc->bycp", sin_y, imag_in, precision=highest
    )
    imag_out = jnp.einsum("ky,pbkc->bycp", sin_y, real_in, precision=highest) + jnp.einsum(
        "ky,pbkc->bycp", cos_y, imag_in, precision=highest
    )
    return jnp.stack([real_out, imag_out], axis=2)


def plane_inverse(spectra, cos_x, sin_x, z_back):
    lead_dims = spectra.shape[:-3]
    values_f = spectra.astype(jnp.float32).reshape(lead_dims + (2, C, MX, MZ))
    real_in = values_f[..., 0, :, :, :]
    imag_in = values_f[..., 1, :, :, :]
    real_out = jnp.einsum("kx,...ckm->...cxm", cos_x, real_in, precision=highest) - jnp.einsum(
        "kx,...ckm->...cxm", sin_x, imag_in, precision=highest
    )
    imag_out = jnp.einsum("kx,...ckm->...cxm", sin_x, real_in, precision=highest) + jnp.einsum(
        "kx,...ckm->...cxm", cos_x, imag_in, precision=highest
    )
    joined = jnp.concatenate([real_out, imag_out], axis=-1)
    result = jnp.dot(
        joined.reshape(-1, 2 * MZ), z_back, precision=highest, preferred_element_type=jnp.float32
    )
    return result.reshape(lead_dims + (C, X, Z)).astype(jnp.bfloat16)


def split_cot(cot_modes):
    real_part = cot_modes[:, :, :, 0]
    imag_part = cot_modes[:, :, :, 1]
    return (
        jnp.concatenate([real_part, imag_part], axis=-1),
        jnp.concatenate([imag_part, -real_part], axis=-1),
    )


def weight_terms(input_modes, cot_modes):
    cot_one, cot_two = split_cot(cot_modes)
    first_term = jnp.einsum(
        "pbki,pbkj->pkij", input_modes[:, :, :, 0], cot_one, preferred_element_type=jnp.float32
    )
    second_term = jnp.einsum(
        "pbki,pbkj->pkij", input_modes[:, :, :, 1], cot_two, preferred_element_type=jnp.float32
    )
    return first_term + second_term


def local_any(inputs, cotangent, mode_weights):
    inv_scale = 1.0 / math.sqrt(X * Y * Z)
    cos_z, sin_z = twiddles(jnp.arange(MZ), jnp.arange(Z), Z)
    z_table = jnp.concatenate([cos_z.T, -sin_z.T], axis=1).astype(jnp.bfloat16)
    z_back = jnp.concatenate([cos_z, -sin_z], axis=0) * inv_scale
    cos_x, sin_x = twiddles(wave_pair(MX, X), jnp.arange(X), X)
    plain_z = jnp.full((MZ,), inv_scale, jnp.float32)
    weight_z = jnp.where(jnp.arange(MZ) == 0, 1.0, 2.0).astype(jnp.float32) * inv_scale
    input_spec = plane_spectrum(inputs, z_table, cos_x, sin_x, plain_z)
    cot_spec = plane_spectrum(cotangent, z_table, cos_x, sin_x, weight_z)
    y_waves = wave_pair(MY, Y)
    positions = jnp.arange(Y)
    cos_y, sin_y = twiddles(y_waves, positions, Y)
    moved_input, moved_cot = (
        lax.all_to_all(input_spec, "space", split_axis=4, concat_axis=1, tiled=True),
        lax.all_to_all(cot_spec, "space", split_axis=4, concat_axis=1, tiled=True),
    )
    input_modes = modes_along_y(moved_input, cos_y, sin_y)
    cot_modes = modes_along_y(moved_cot, cos_y, sin_y)
    input_modes = input_modes.astype(jnp.bfloat16)
    cot_modes = cot_modes.astype(jnp.bfloat16)
    weight_grad = lax.psum(
        weight_terms(input_modes, cot_modes).astype(jnp.bfloat16), "batch"
    ).astype(jnp.float32)
    cot_one, cot_two = split_cot(cot_modes)
    grad_real = jnp.einsum(
        "pbkj,pkij->pbki", cot_one, mode_weights, preferred_element_type=jnp.float32
    )
    grad_imag = jnp.einsum(
        "pbkj,pkij->pbki", cot_two, mode_weights, preferred_element_type=jnp.float32
    )
    mode_grad = jnp.stack([grad_real, grad_imag], axis=3).astype(jnp.bfloat16)
    plane_modes = planes_along_y(mode_grad, cos_y, sin_y).astype(jnp.bfloat16)
    back_spec = lax.all_to_all(plane_modes, "space", split_axis=1, concat_axis=4, tiled=True)
    input_grad = plane_inverse(back_spec, cos_x, sin_x, z_back)
    return (input_grad, weight_grad)


GROUP = 8
QUAD = 4
ROWS = 16
LANES = 128
BLOCK = 4
STEP = 4


def angles_of(waves, length):
    turns = 2.0 * np.pi / length * (np.outer(waves, np.arange(length)) % length)
    return np.cos(turns), np.sin(turns)


def signed_waves(retained, length):
    return np.concatenate([np.arange(retained // 2), np.arange(length - retained // 2, length)])


def as_table(array):
    return np.asarray(array, np.float32).astype(jnp.bfloat16)


def x_tables(length):
    cos_x, sin_x = angles_of(signed_waves(MX, length), length)
    both = np.stack([cos_x, sin_x])
    forward = np.einsum("qkx,cd->qkcdx", both, np.eye(QUAD))
    forward = forward.reshape(2 * MX * QUAD, QUAD * length)
    unit = np.eye(GROUP)
    both = np.stack([cos_x, -sin_x])
    back = np.einsum("qkx,cd->dxqkc", both, unit).reshape(GROUP * length, 2 * MX * GROUP)
    return as_table(forward), as_table(back)


def z_tables(length, scale):
    cos_z, sin_z = angles_of(np.arange(MZ), length)
    forward = np.concatenate(
        [np.concatenate([cos_z, -sin_z], axis=1), np.concatenate([-sin_z, -cos_z], axis=1)]
    )
    doubled = np.where(np.arange(MZ) == 0, 1.0, 2.0)[:, None]
    doubled = np.concatenate([doubled, doubled])
    back = np.concatenate(
        [np.concatenate([cos_z, sin_z], axis=1), np.concatenate([-sin_z, cos_z], axis=1)]
    )
    rounded = as_table(forward).astype(np.float32) * scale
    return as_table(rounded.T), as_table((rounded * doubled).T), as_table(back * scale)


def lane_table(waves, channels):
    table = np.zeros((waves * channels, waves * channels))
    for wave in range(waves):
        for channel in range(channels):
            group, place = divmod(channel, QUAD)
            table[(group * waves + wave) * QUAD + place, wave * channels + channel] = 1.0
    return as_table(table)


def y_tables(length, shards):
    cos_y, sin_y = angles_of(signed_waves(MY, length), length)
    per = length // shards
    real = np.stack([cos_y, sin_y], axis=1)
    imag = np.stack([-sin_y, cos_y], axis=1)
    rows = np.stack([real, imag], axis=1).reshape(2 * MY, 2, shards, per)
    forward = rows.transpose(2, 0, 1, 3).reshape(shards, 2 * MY, 2 * per)
    back = np.stack([np.stack([cos_y, -sin_y], axis=-1), np.stack([sin_y, cos_y], axis=-1)])
    back = back.transpose(2, 0, 1, 3).reshape(shards, 2 * per, 2 * MY)
    return as_table(forward), as_table(back)


def peer_order(bits):
    if not bits:
        return [0]
    kept = peer_order(bits[1:])
    return kept + [distance ^ bits[0] for distance in kept]


def gathered_order(bits):
    held = [0]
    for bit in bits:
        held = held + [distance ^ bit for distance in held]
    return held


def dot(left, right, left_dim=1, right_dim=0):
    dims = (((left_dim,), (right_dim,)), ((), ()))
    return lax.dot_general(left, right, dims, preferred_element_type=jnp.float32)


def spectrum_kernel(block, orders, me_ref, field_ref, x_ref, z_ref, y_ref, lane_ref, *refs):
    *part_refs, field_buf, rows_ref, total_ref, sems = refs
    planes, channels, length, depth = field_buf.shape
    shards, _, width = total_ref.shape

    def incoming(plane):
        return pltpu.make_async_copy(field_ref.at[0, plane], field_buf.at[plane], sems.at[plane])

    for plane in range(planes):
        incoming(plane).start()

    @pl.loop(0, planes // block)
    def _(step):
        for place in range(block):
            incoming(step * block + place).wait()
        for place in range(block):
            plane = step * block + place
            for first in range(0, channels, 2 * QUAD):
                sides = [
                    field_buf[plane, first + side * QUAD : first + (side + 1) * QUAD].reshape(
                        QUAD * length, depth
                    )
                    for side in range(2)
                ]
                mixed = dot(x_ref[...], jnp.concatenate(sides, axis=1))
                half = MX * QUAD
                parts = [
                    jnp.concatenate(
                        [
                            mixed[:half, side * depth : (side + 1) * depth],
                            mixed[half:, side * depth : (side + 1) * depth],
                        ],
                        axis=1,
                    ).reshape(shards, half // shards, 2 * depth)
                    for side in range(2)
                ]
                rows = half // shards
                start = first // QUAD * rows
                rows_ref[place, :, start : start + 2 * rows, :] = jnp.concatenate(
                    parts, axis=1
                ).astype(jnp.bfloat16)
            for shard in range(shards):
                modes = dot(rows_ref[place, shard], z_ref[...])
                total_ref[shard, pl.ds(plane, 2 * MZ, stride=planes), :] = modes.T

    me = me_ref[0]
    table = y_ref[me]
    chunk = MZ // len(orders)
    for stream, order in enumerate(orders):
        for kz in range(chunk):
            first = (stream * chunk + kz) * planes
            pieces = [
                total_ref[me ^ distance, pl.ds(part * MZ * planes + first, planes), :]
                for distance in order
                for part in range(2)
            ]
            moved = jnp.concatenate(pieces).astype(jnp.bfloat16)
            moved = dot(moved, lane_ref[...]).astype(jnp.bfloat16)
            rows = 2 * planes
            parts = [moved[place * rows : (place + 1) * rows] for place in range(shards)]
            modes = dot(table, jnp.concatenate(parts, axis=1)).astype(jnp.bfloat16)
            for place in range(shards):
                side, place_in = divmod(place, shards // 2)
                part_refs[2 * stream + side][place_in, kz] = modes[
                    :, place * width : (place + 1) * width
                ]


def plane_modes(me, field, x_table, z_table, y_table, lanes, orders, block):
    _, planes, channels, length, depth = field.shape
    shards = len(orders[0])
    width = MX * channels // shards
    shape = (shards // 2, MZ // len(orders), 2 * MY, width)
    vmem = pl.BlockSpec(memory_space=pltpu.VMEM)
    return pl.pallas_call(
        functools.partial(spectrum_kernel, block, orders),
        out_shape=[jax.ShapeDtypeStruct(shape, jnp.bfloat16)] * (2 * len(orders)),
        in_specs=[
            pl.BlockSpec(memory_space=pltpu.SMEM),
            pl.BlockSpec(memory_space=pl.ANY),
            vmem,
            vmem,
            vmem,
            vmem,
        ],
        out_specs=[vmem] * (2 * len(orders)),
        scratch_shapes=[
            pltpu.VMEM((planes, channels, length, depth), jnp.bfloat16),
            pltpu.VMEM((block, shards, width, 2 * depth), jnp.bfloat16),
            pltpu.VMEM((shards, 2 * MZ * planes, width), jnp.float32),
            pltpu.SemaphoreType.DMA((planes,)),
        ],
        cost_estimate=pl.CostEstimate(
            flops=2 * field.size * 8 * MX, bytes_accessed=2 * field.size, transcendentals=0
        ),
        name="plane_modes",
    )(me, field, x_table, z_table, y_table, lanes)


def swapped(array, bit, shards):
    return lax.ppermute(array, "space", [(i, i ^ bit) for i in range(shards)])


def total(keep, moved):
    return (keep.astype(jnp.float32) + moved.astype(jnp.float32)).astype(jnp.bfloat16)


def halved(keep, moved):
    both = total(keep, moved)
    half = both.shape[0] // 2
    return both[:half], both[half:]


def after(values):
    return lax.optimization_barrier(values)


def turned_rows(modes):
    rows = modes.shape[0]
    row = lax.broadcasted_iota(jnp.int32, modes.shape, 0)
    return jnp.where(row % 2 == 0, pltpu.roll(modes, rows - 1, 0), -pltpu.roll(modes, 1, 0))


def join_halves(plain, turned, side):
    low = lax.broadcasted_iota(jnp.int32, plain.shape, 1) < LANES // 2
    if side == 0:
        return jnp.where(low, plain, pltpu.roll(turned, LANES // 2, 1))
    return jnp.where(low, pltpu.roll(plain, LANES // 2, 1), turned)


def mode_grad_kernel(keep_ref, moved_ref, w_ref, *refs):
    *_, modes_ref, grad_ref = refs
    _, chunk, _, channels, _ = w_ref.shape
    row = lax.broadcasted_iota(jnp.int32, (2 * MY, MY * channels), 0) // 2
    lane = lax.broadcasted_iota(jnp.int32, (2 * MY, MY * channels), 1) // channels
    own = row == lane
    low = lax.broadcasted_iota(jnp.int32, (2 * MY, LANES), 1) < LANES // 2
    for kz in range(chunk):
        plain = keep_ref[0, kz].astype(jnp.float32) + moved_ref[0, kz].astype(jnp.float32)
        turned = turned_rows(plain)
        modes_ref[kz] = plain.astype(jnp.bfloat16)
        sides = []
        for side in range(2):
            left = join_halves(plain, turned, side).astype(jnp.bfloat16)
            crossed = dot(left, w_ref[side, kz].reshape(MY * channels, 2 * channels), 1, 1)
            crossed = jnp.where(own, crossed, 0.0)
            kept = crossed[:, :LANES]
            for first in range(LANES, MY * channels, LANES):
                kept = kept + crossed[:, first : first + LANES]
            sides.append(kept + pltpu.roll(kept, LANES // 2, 1))
        grad_ref[0, kz] = jnp.where(low, sides[0], sides[1]).astype(jnp.bfloat16)


def mode_grads(keep, moved, weights, modes, first, chunk):
    _, kinds, rows, width = keep.shape
    channels = weights.shape[3]
    part_spec = pl.BlockSpec((1, chunk, rows, width), lambda i: (0, i, 0, 0))
    return pl.pallas_call(
        mode_grad_kernel,
        out_shape=(
            jax.ShapeDtypeStruct((MZ, rows, width), jnp.bfloat16),
            jax.ShapeDtypeStruct(keep.shape, jnp.bfloat16),
        ),
        grid=(kinds // chunk,),
        in_specs=[
            part_spec,
            part_spec,
            pl.BlockSpec(
                (2, chunk, MY, channels, 2 * channels), lambda i: (0, i + first // chunk, 0, 0, 0)
            ),
        ]
        + [pl.BlockSpec(memory_space=pl.ANY)] * len(modes),
        out_specs=(
            pl.BlockSpec((chunk, rows, width), lambda i: (i + first // chunk, 0, 0)),
            part_spec,
        ),
        input_output_aliases={3: 0} if modes else {},
        compiler_params=pltpu.CompilerParams(dimension_semantics=("arbitrary",)),
        cost_estimate=pl.CostEstimate(
            flops=4 * MY * weights.size, bytes_accessed=weights.size, transcendentals=0
        ),
        name="mode_grads",
    )(keep, moved, weights, *modes)


def weight_kernel(channels, *refs):
    *mode_refs, out_ref = refs
    samples = len(mode_refs) // 2
    for kz in range(out_ref.shape[1]):
        inputs = jnp.concatenate([ref[kz] for ref in mode_refs[:samples]]).astype(jnp.float32)
        cots = jnp.concatenate([ref[kz] for ref in mode_refs[samples:]]).astype(jnp.float32)
        turned = turned_rows(cots)
        wave = lax.broadcasted_iota(jnp.int32, cots.shape, 0) % (2 * MY) // 2
        left = inputs.T.astype(jnp.bfloat16)
        for side in range(2):
            right = join_halves(cots, turned, side)
            mine = left[side * channels : (side + 1) * channels]
            for ky in range(0, MY, 2):
                pair = [jnp.where(wave == ky + k, right, 0.0).astype(jnp.bfloat16) for k in range(2)]
                grads = dot(mine, jnp.concatenate(pair, axis=1))
                for k in range(2):
                    out_ref[side, kz, ky + k] = grads[:, k * LANES : (k + 1) * LANES]


def weight_grads(input_modes, cot_modes, channels, chunk):
    samples = len(input_modes)
    kinds, rows, width = input_modes[0].shape
    shape = (2, kinds, MY, channels, 2 * channels)
    return pl.pallas_call(
        functools.partial(weight_kernel, channels),
        out_shape=jax.ShapeDtypeStruct(shape, jnp.float32),
        grid=(kinds // chunk,),
        in_specs=[pl.BlockSpec((chunk, rows, width), lambda i: (i, 0, 0))] * (2 * samples),
        out_specs=pl.BlockSpec((2, chunk, MY, channels, 2 * channels), lambda i: (0, i, 0, 0, 0)),
        compiler_params=pltpu.CompilerParams(dimension_semantics=("arbitrary",)),
        cost_estimate=pl.CostEstimate(
            flops=2 * 128 * math.prod(shape), bytes_accessed=4 * math.prod(shape), transcendentals=0
        ),
        name="weight_grads",
    )(*input_modes, *cot_modes)


def inverse_kernel(orders, me_ref, *refs):
    *held_refs, y_ref, z_ref, x_ref, out_ref, total_ref = refs
    step = pl.program_id(0)
    block, channels, length, depth = out_ref.shape[1:]
    shards, _, width = total_ref.shape

    @pl.when(step == 0)
    def _():
        me = me_ref[0]
        table = y_ref[me]
        chunk = MZ // len(orders)
        count = len(held_refs) // len(orders)
        for stream, order in enumerate(orders):
            for kz in range(chunk):
                modes = jnp.concatenate(
                    [
                        ref[place, kz]
                        for ref in held_refs[stream * count : (stream + 1) * count]
                        for place in range(ref.shape[0])
                    ],
                    axis=1,
                )
                spread = dot(table, modes)
                for place, distance in enumerate(order):
                    rows = pl.ds(stream * chunk + kz, table.shape[0], stride=MZ)
                    total_ref[me ^ distance, rows, :] = spread[
                        :, place * width : (place + 1) * width
                    ]

    for plane in range(block):
        rows = pl.ds((step * block + plane) * 2 * MZ, 2 * MZ)
        modes = jnp.concatenate([total_ref[shard, rows, :] for shard in range(shards)], axis=1)
        modes = modes.astype(jnp.bfloat16)
        along = dot(modes, z_ref[...], 0, 0).reshape(MX, channels, 2 * depth)
        for first in range(0, channels, 2 * GROUP):
            sides = []
            for side in range(2):
                start = first + side * GROUP
                piece = along[:, start : start + GROUP].reshape(MX * GROUP, 2 * depth)
                sides.append(jnp.concatenate([piece[:, :depth], piece[:, depth:]], axis=0))
            grads = dot(x_ref[...], jnp.concatenate(sides, axis=1).astype(jnp.bfloat16))
            for side in range(2):
                start = first + side * GROUP
                out_ref[0, plane, start : start + GROUP] = (
                    grads[:, side * depth : (side + 1) * depth]
                    .reshape(GROUP, length, depth)
                    .astype(jnp.bfloat16)
                )


def plane_grads(me, held, y_back, z_back, x_back, orders, shape, block):
    _, planes, channels, length, depth = shape
    shards = len(orders[0])
    width = held[0].shape[-1]
    return pl.pallas_call(
        functools.partial(inverse_kernel, orders),
        out_shape=jax.ShapeDtypeStruct(shape, jnp.bfloat16),
        grid=(planes // block,),
        in_specs=[pl.BlockSpec(memory_space=pltpu.SMEM)]
        + [pl.BlockSpec(array.shape, lambda i: (0, 0, 0, 0)) for array in held]
        + [
            pl.BlockSpec(y_back.shape, lambda i: (0, 0, 0)),
            pl.BlockSpec(z_back.shape, lambda i: (0, 0)),
            pl.BlockSpec(x_back.shape, lambda i: (0, 0)),
        ],
        out_specs=pl.BlockSpec((1, block, channels, length, depth), lambda i: (0, i, 0, 0, 0)),
        scratch_shapes=[pltpu.VMEM((shards, planes * 2 * MZ, width), jnp.float32)],
        compiler_params=pltpu.CompilerParams(dimension_semantics=("arbitrary",)),
        cost_estimate=pl.CostEstimate(
            flops=2 * math.prod(shape) * 8 * MX,
            bytes_accessed=2 * math.prod(shape),
            transcendentals=0,
        ),
        name="plane_grads",
    )(me, *held, y_back, z_back, x_back)


def from_peers(array, groups):
    held = [array]
    for bit in [1 << place for place in range(groups.bit_length() - 1)][::-1]:
        pairs = [(i, i ^ bit) for i in range(groups)]
        held = held + [lax.ppermute(one, "batch", pairs) for one in held]
    return held


def local_fast(shards, groups, inputs, cotangent, mode_weights):
    _, planes, channels, length, depth = inputs.shape
    scale = 1.0 / math.sqrt(length * planes * shards * depth)
    x_table, x_back = x_tables(length)
    z_plain, z_double, z_back = z_tables(depth, scale)
    y_table, y_back = y_tables(planes * shards, shards)
    lanes = lane_table(MX // shards, channels)
    me = lax.axis_index("space").reshape(1)
    bits = [1 << place for place in range(shards.bit_length() - 1)]
    paths = [bits, [bits[1], bits[0]] + bits[2:]]
    down = [peer_order(path) for path in paths]
    up = [gathered_order(path[::-1]) for path in paths]
    streams = range(len(paths))

    def split(parts):
        return [parts[2 * k] for k in streams], [parts[2 * k + 1] for k in streams]

    def reduce_step(keep, moved):
        pairs = [halved(keep[k], moved[k]) for k in streams]
        return [pair[0] for pair in pairs], [pair[1] for pair in pairs]

    def swap_all(arrays, routes, step):
        moved = []
        for k in streams:
            moved.append(swapped(arrays[k], routes[k][step], shards))
        return moved

    keep, send = split(plane_modes(me, cotangent, x_table, z_double, y_table, lanes, down, BLOCK))
    moved = swap_all(send, paths, 0)
    parts = plane_modes(me, inputs, x_table, z_plain, y_table, lanes, down, BLOCK)
    moved, parts = after((moved, parts))
    input_keep, input_send = split(parts)
    input_moved, input_sends = None, 0
    for step in range(1, len(bits)):
        keep, send = reduce_step(keep, moved)
        if input_moved is None:
            send, input_send = after((send, input_send))
        else:
            send, input_moved = after((send, input_moved))
            input_keep, input_send = reduce_step(input_keep, input_moved)
        moved = swap_all(send, paths, step)
        input_moved = swap_all(input_send, paths, input_sends)
        input_sends += 1
    weights = mode_weights.reshape(2, MZ, MY, channels, 2 * channels)
    chunk = MZ // len(paths)
    routes = [path[::-1] for path in paths]
    cot_modes, held, came = [], [], []
    for k in streams:
        if k:
            input_keep, input_send = reduce_step(input_keep, input_moved)
            input_moved = swap_all(input_send, paths, input_sends)
        keep[k], input_send = after((keep[k], input_send))
        modes, grad = mode_grads(keep[k], moved[k], weights, cot_modes, k * chunk, STEP)
        cot_modes = [modes]
        held.append([grad])
        came.append(swapped(grad, routes[k][0], shards))
    input_modes = jnp.concatenate([total(input_keep[k][0], input_moved[k][0]) for k in streams])
    input_modes, came = after((input_modes, came))
    all_cots = from_peers(cot_modes[0], groups)
    all_inputs = from_peers(input_modes, groups)
    came = [[array] for array in came]
    for step in range(1, len(bits)):
        held = [[jnp.concatenate(held[k] + came[k])] for k in streams]
        came = [[array] for array in swap_all([one[0] for one in held], routes, step)]
    all_inputs, held = after((all_inputs, held))
    weight_grad = weight_grads(all_inputs, all_cots, channels, STEP)
    came, weight_grad = after((came, weight_grad))
    gathered = [array for k in streams for array in held[k] + came[k]]
    input_grad = plane_grads(me, gathered, y_back, z_back, x_back, up, inputs.shape, BLOCK)
    return (input_grad, weight_grad.reshape(mode_weights.shape))


def local(shards, groups, inputs, cotangent, mode_weights):
    samples, planes, channels, _, depth = inputs.shape
    fits = (
        samples == 1
        and planes % ROWS == 0
        and MX % shards == 0
        and MX // shards * channels == LANES
        and depth == LANES
        and shards > 2
        and shards & (shards - 1) == 0
        and groups & (groups - 1) == 0
    )
    if fits:
        return local_fast(shards, groups, inputs, cotangent, mode_weights)
    return local_any(inputs, cotangent, mode_weights)


def solution(mesh):
    placed = (
        P("batch", "space", None, None, None),
        P("batch", "space", None, None, None),
        P("space", None, None, None),
    )
    return jax.shard_map(
        functools.partial(local, mesh.shape["space"], mesh.shape["batch"]),
        mesh=mesh,
        in_specs=placed,
        out_specs=(P("batch", "space", None, None, None), P("space", None, None, None)),
        check_vma=False,
    )
```
